32 devices in a mesh: dom: 8 (over y, x, core), feat: 4 (over z).
Axes of the slice: x: 2, y: 2, z: 4, core: 2. Of those that a mesh axis runs over, the one named last changes fastest.
Arguments:
- features: bfloat16 [512, 65536], P('feat', 'dom'), may hold values from -3 to 3
- send_blocks: int32 [8, 8, 8], P('dom'), may hold values from 0 to 63, as said below
- counts: int32 [8, 8], P('dom'), may hold values from 0 to 8, as said below
- tile_blocks: int32 [24, 512], P(None, 'dom'), may hold values from 0 to 127, as said below
- neighbours: int32 [24, 65536], P(None, 'dom'), may hold values from 0 to 127
- degree: int32 [65536], P('dom'), may hold values from 1 to 24
- epsilon: float32 [1], replicated, may hold values from -0.3 to 0.6
- w_first: bfloat16 [512, 512], replicated, may hold values from -0.25 to 0.25
- b_first: float32 [512], replicated, may hold values from -3 to 3
- w_second: bfloat16 [512, 512], replicated, may hold values from -0.25 to 0.25
- b_second: float32 [512], replicated, may hold values from -3 to 3
Outputs:
- updated: bfloat16 [65536, 512], P(('dom', 'feat'))
The draws below stay inside these ranges and needn't reach their ends.
Inputs may be any that keep to these rules, and one draw needn't show every extreme that they name: `send_blocks`: entry [q, p, s] is a row block of partition q; the entries of one pair (q, p) are distinct. counts[q, p] leading slots of send_blocks[q, p] are used; zero where q == p; in every draw some partition receives 8 blocks from every other partition. `tile_blocks`: an entry for a row block of partition p is below 64 (a row block of p) or equals 64 + q * 8 + s for a slot s of a partition q other than p.
All inputs are finite; a program needn't handle non-finite values.
Results may differ from the reference program's by a relative error of at most 0.0055.
Values may be sent and summed in bfloat16 or wider, within the bound.
A program may use at most 64 MiB of HBM per device.

```python
import jax
import jax.numpy as jnp
from jax import lax

D = 512
H = 512
ROWS = 8192
BLOCK = 128
SLOTS = 8
NEIGH = 24
PARTITIONS = 8
NODES = 65536
BLOCKS = 64


def draw_send_blocks(key, part):
    key_list = jax.random.split(jax.random.fold_in(key, 11), PARTITIONS * PARTITIONS)

    def pick(single):
        return jax.random.permutation(single, BLOCKS)[:SLOTS]
    picked = jax.vmap(pick)(key_list)
    return picked.reshape(PARTITIONS, PARTITIONS, SLOTS).astype(jnp.int32)


def draw_counts(key, part):
    first, second = jax.random.split(jax.random.fold_in(key, 23))
    base = jax.random.randint(first, (PARTITIONS, PARTITIONS), 1, SLOTS + 1)
    heavy = jax.random.randint(second, (), 0, PARTITIONS)
    column = jnp.arange(PARTITIONS, dtype=jnp.int32)[None, :]
    rowpos = jnp.arange(PARTITIONS, dtype=jnp.int32)[:, None]
    base = jnp.where(column == heavy, SLOTS, base)
    base = jnp.where(column == rowpos, 0, base)
    return base.astype(jnp.int32)


def draw_tile_blocks(key, part):
    keys = jax.random.split(jax.random.fold_in(key, 37), 4)
    block_count = NODES // BLOCK
    shape = (block_count, NEIGH)
    dst_part = (jnp.arange(block_count, dtype=jnp.int32) // BLOCKS)[:, None]
    which = jax.random.randint(keys[0], shape, 0, 2)
    local = jax.random.randint(keys[1], shape, 0, BLOCKS)
    source = (dst_part + jax.random.randint(keys[2], shape, 1, PARTITIONS)) % PARTITIONS
    slot_pick = jax.random.randint(keys[3], shape, 0, SLOTS)
    remote = BLOCKS + source * SLOTS + slot_pick
    return jnp.where(which == 0, local, remote).astype(jnp.int32).T


def set_ends(entries, key, least, high):
    spot = [jax.random.randint(jax.random.fold_in(key, axis), (), 0, length) for axis, length in enumerate(entries.shape)]
    longest = entries.shape.index(max(entries.shape))
    beside = spot[:longest] + [(spot[longest] + 1) % entries.shape[longest]] + spot[longest + 1:]
    return entries.at[tuple(spot)].set(least).at[tuple(beside)].set(high)


def block_levels(rng, dims, pieces, low, largest):
    gain = 1.0
    for dim, shards_of in pieces:
        draws = jax.random.uniform(jax.random.fold_in(jax.random.fold_in(rng, 6), dim), (shards_of,), jnp.float32, low / len(pieces), largest / len(pieces))
        gain = gain * jnp.repeat(jnp.exp(draws), dims[dim] // shards_of).reshape((-1,) + (1,) * (len(dims) - 1 - dim))
    return gain


def noise(own_key, extent, spread, bound, cuts=(), kind=jnp.bfloat16):
    result = jax.random.normal(own_key, extent, jnp.float32) * spread
    if len(cuts) > 0:
        result = block_levels(own_key, extent, cuts, -0.22, 0.18) * result
    return jnp.clip(result, min=-bound, max=bound).astype(kind)


def setup_inputs(seed: int = 0) -> dict:
    streams_of = jax.random.split(jax.random.key(seed), 12)
    features = noise(streams_of[0], (D, NODES), 0.5, 3.0, ((0, 4), (1, 8)))
    send_blocks = draw_send_blocks(jax.random.fold_in(streams_of[11], 71), 0)
    counts = draw_counts(jax.random.fold_in(streams_of[11], 71), 0)
    tile_blocks = draw_tile_blocks(jax.random.fold_in(streams_of[11], 71), 0)
    neighbours = set_ends(jax.random.randint(streams_of[4], (NEIGH, NODES), 0, BLOCK), jax.random.fold_in(streams_of[4], 1), 0, BLOCK - 1).astype(jnp.int32)
    degree = set_ends(jax.random.randint(streams_of[5], (NODES,), 1, NEIGH + 1), jax.random.fold_in(streams_of[5], 1), 1, NEIGH).astype(jnp.int32)
    epsilon = jnp.clip(jax.random.uniform(streams_of[6], (1,), jnp.float32, -0.3, 0.6), -0.3, 0.6)
    w_first = noise(streams_of[7], (D, H), D ** -0.5, 0.25)
    b_first = noise(streams_of[8], (H,), 0.5, 3.0, (), jnp.float32)
    w_second = noise(streams_of[9], (H, D), H ** -0.5, 0.25)
    b_second = noise(streams_of[10], (D,), 0.5, 3.0, (), jnp.float32)
    return {"features": features, "send_blocks": send_blocks, "counts": counts, "tile_blocks": tile_blocks, "neighbours": neighbours, "degree": degree, "epsilon": epsilon, "w_first": w_first, "b_first": b_first, "w_second": w_second, "b_second": b_second}


def reference(features, send_blocks, counts, tile_blocks, neighbours, degree, epsilon, w_first, b_first, w_second, b_second):
    node_rows = features.T
    tile_rows = jnp.repeat(tile_blocks.T, BLOCK, axis=0)
    lists = (tile_rows * BLOCK + neighbours.T).astype(jnp.int32)
    row_ids = jnp.arange(NODES, dtype=jnp.int32)
    row_part = (row_ids // ROWS)[:, None]
    offset = jnp.maximum(lists - ROWS, 0)
    source = offset // (SLOTS * BLOCK)
    slot_index = (offset // BLOCK) % SLOTS
    in_block = offset % BLOCK
    block_index = send_blocks[source, row_part, slot_index]
    remote = source * ROWS + block_index * BLOCK + in_block
    is_local = lists < ROWS
    target = jnp.where(is_local, row_part * ROWS + lists, remote).astype(jnp.int32)
    live_mask = (jnp.arange(NEIGH, dtype=jnp.int32)[None, :] < degree[:, None]) & (is_local | (slot_index < counts[source, row_part]))
    weight = live_mask.astype(jnp.float32)
    block_rows = min(NODES, 4096)

    def block_sum(pair):
        gathered = node_rows[pair[0]].astype(jnp.float32)
        return jnp.einsum('rk,rkd->rd', pair[1], gathered)

    near_sum = lax.map(block_sum, (target.reshape(-1, block_rows, NEIGH), weight.reshape(-1, block_rows, NEIGH)))
    near_sum = near_sum.reshape(NODES, D)
    combined = ((1.0 + epsilon[0]) * node_rows.astype(jnp.float32) + near_sum).astype(jnp.bfloat16)
    pre_act = jnp.dot(combined, w_first, preferred_element_type=jnp.float32) + b_first
    activated = jax.nn.relu(pre_act).astype(jnp.bfloat16)
    return (jnp.dot(activated, w_second, preferred_element_type=jnp.float32) + b_second).astype(jnp.bfloat16)
```

```python
import functools

import jax
import jax.numpy as jnp
from jax import lax
from jax.experimental import pallas as pl
from jax.experimental.pallas import tpu as pltpu
from jax.sharding import PartitionSpec as P

BLOCK = 128
SUBLANES = 16
PIECES = 4


def chunk_widths(cols):
    widths = []
    while sum(widths) < cols:
        widths.append(min(max(SUBLANES, sum(widths)), cols - sum(widths)))
    return widths


def kernel(
    parts, groups, pieces, widths,
    sb_hbm, cnt_hbm, tile_hbm, eps_ref, deg_hbm, b1_hbm, b2_hbm,
    feat_hbm, nbr_hbm, w1_hbm, w2_hbm,
    out_ref,
    *scratch,
):
    chunks = len(widths)
    starts = [sum(widths[:c]) for c in range(chunks)]
    tables, locals_, stages, feats = (scratch[i * chunks:(i + 1) * chunks] for i in range(4))
    (sb_ref, cnt_ref, tile_ref, deg_ref, b1_ref, b2_ref,
     nbr_ref, w1_ref, w2_ref, zstage, parcel,
     hsend, hrecv, zsend, zrecv, in_sem) = scratch[4 * chunks:]
    me = lax.axis_index("dom")
    z = lax.axis_index("feat")
    slots = stages[0].shape[1]
    list_width, block_count = tile_ref.shape
    per_piece = block_count // groups // pieces
    piece_nodes = per_piece * BLOCK
    half = groups // 2

    def lanes(block):
        return pl.ds(pl.multiple_of(block * BLOCK, BLOCK), BLOCK)

    def halo_copy(c, peer, source):
        return pltpu.make_async_remote_copy(
            src_ref=stages[c].at[peer],
            dst_ref=tables[c].at[pl.ds(block_count + source * slots, slots)],
            send_sem=hsend.at[0],
            recv_sem=hrecv.at[c],
            device_id={"dom": peer},
            device_id_type=pl.DeviceIdType.MESH,
        )

    def row_copy(c, p, dest, source):
        span = pl.ds(starts[c], widths[c])
        return pltpu.make_async_remote_copy(
            src_ref=zstage.at[p, dest, span],
            dst_ref=parcel.at[p, source, span],
            send_sem=zsend.at[0],
            recv_sem=zrecv.at[p],
            device_id={"feat": dest},
            device_id_type=pl.DeviceIdType.MESH,
        )

    def halo_all(c, sem):
        blocks = tables[c].at[pl.ds(0, (parts - 1) * slots)]
        return pltpu.make_async_copy(blocks, blocks, sem)

    def row_all(p, sem):
        rows = parcel.at[p, pl.ds(0, groups - 1)]
        return pltpu.make_async_copy(rows, rows, sem)

    def dest_of(k):
        if k < half:
            return lax.rem(z // half + 1, 2) * half + lax.rem(lax.rem(z, half) + k, half)
        return (z // half) * half + lax.rem(lax.rem(z, half) + (k - half + 1), half)

    barrier = pltpu.get_barrier_semaphore()

    @pl.loop(1, parts)
    def _(k):
        pl.semaphore_signal(
            barrier, inc=1, device_id={"dom": lax.rem(me + k, parts)},
            device_id_type=pl.DeviceIdType.MESH,
        )

    @pl.loop(1, groups)
    def _(k):
        pl.semaphore_signal(
            barrier, inc=1, device_id={"feat": lax.rem(z + k, groups)},
            device_id_type=pl.DeviceIdType.MESH,
        )

    loads = [
        pltpu.make_async_copy(
            feat_hbm.at[pl.ds(starts[c], widths[c])], feats[c], in_sem.at[c]
        )
        for c in range(chunks)
    ]
    small = [
        pltpu.make_async_copy(source, target, in_sem.at[chunks])
        for source, target in ((sb_hbm, sb_ref), (cnt_hbm, cnt_ref))
    ]
    lists = [
        pltpu.make_async_copy(source, target, in_sem.at[chunks + 1])
        for source, target in (
            (tile_hbm, tile_ref), (deg_hbm, deg_ref), (nbr_hbm, nbr_ref),
        )
    ]
    weights = [
        pltpu.make_async_copy(source, target, in_sem.at[chunks + 2])
        for source, target in (
            (w1_hbm, w1_ref), (w2_hbm, w2_ref), (b1_hbm, b1_ref), (b2_hbm, b2_ref),
        )
    ]
    for load in loads[:1] + small + loads[1:] + lists + weights:
        load.start()
    for load in small:
        load.wait()

    for c in range(chunks):
        loads[c].wait()

        @pl.loop(0, block_count, unroll=4)
        def _(b):
            block = feats[c][:, lanes(b)]
            locals_[c][b] = block
            tables[c][b] = block

        if c == 0:
            pl.semaphore_wait(barrier, parts + groups - 2)

        @pl.loop(1, parts)
        def _(k):
            peer = lax.rem(me + k, parts)
            for s in range(slots):
                used = (s < cnt_ref[0, peer]).astype(jnp.float32)
                block = locals_[c][sb_ref[0, peer, s]]
                stages[c][peer, s] = (block.astype(jnp.float32) * used).astype(jnp.bfloat16)
            halo_copy(c, peer, me).start()

    for c in range(chunks):
        tables[c][pl.ds(block_count + me * slots, slots)] = jnp.zeros(
            (slots, widths[c], BLOCK), jnp.bfloat16
        )

    for load in lists:
        load.wait()
    gain = 1.0 + eps_ref[0]

    def mixed_block(c, b):
        shape = (widths[c], BLOCK)
        total = gain * feats[c][:, lanes(b)].astype(jnp.float32)
        near = jnp.zeros(shape, jnp.float32)
        degree = jnp.broadcast_to(deg_ref[pl.ds(b, 1), :], shape)
        for j in range(list_width):
            tile = tables[c][tile_ref[j, b]].astype(jnp.float32)
            index = jnp.broadcast_to(nbr_ref[pl.ds(j, 1), lanes(b)], shape)
            taken = jnp.take_along_axis(tile, index, axis=1, mode="promise_in_bounds")
            near = near + jnp.where(degree > j, taken, 0.0)
        return (total + near).astype(jnp.bfloat16)

    for c in range(chunks):
        halo_all(c, hrecv.at[c]).wait()

        span = pl.ds(starts[c], widths[c])
        unroll = per_piece if widths[c] <= 2 * SUBLANES else max(per_piece // 2, 1)

        @pl.loop(0, pieces)
        def _(p):
            for k in range(groups):
                dest = dest_of(k) if k < groups - 1 else z
                first = (dest * pieces + p) * per_piece

                @pl.loop(0, per_piece, unroll=unroll)
                def _(i):
                    block = mixed_block(c, first + i)
                    if k < groups - 1:
                        zstage[p, dest, span, lanes(i)] = block
                    else:
                        parcel[p, z, span, lanes(i)] = block

                if k < groups - 1:
                    row_copy(c, p, dest, z).start()

    for load in weights:
        load.wait()
    for c in range(chunks):
        halo_all(c, hsend.at[0]).wait()
    depth = w1_ref.shape[0]

    @pl.loop(0, pieces)
    def _(p):
        row_all(p, zrecv.at[p]).wait()
        columns = parcel[p].reshape(depth, piece_nodes)
        hidden = lax.dot_general(
            columns, w1_ref[...], (((0,), (0,)), ((), ())), preferred_element_type=jnp.float32
        ) + b1_ref[...]
        hidden = jnp.maximum(hidden, 0.0).astype(jnp.bfloat16)
        rows = pl.ds(pl.multiple_of(p * piece_nodes, piece_nodes), piece_nodes)
        out_ref[rows, :] = (
            jnp.dot(hidden, w2_ref[...], preferred_element_type=jnp.float32) + b2_ref[...]
        ).astype(jnp.bfloat16)

    for p in range(pieces):
        row_all(p, zsend.at[0]).wait()


def per_device(
    features, send_blocks, counts, tile_blocks, neighbours, degree, epsilon,
    w_first, b_first, w_second, b_second,
):
    parts = lax.axis_size("dom")
    groups = lax.axis_size("feat")
    cols, rows = features.shape
    slots = send_blocks.shape[2]
    widths = chunk_widths(cols)
    chunks = len(widths)
    block_count = rows // BLOCK
    owned = rows // groups
    pieces = min(PIECES, owned // BLOCK)
    hidden_cols, out_cols = w_second.shape
    depth = w_first.shape[0]
    vmem = pl.BlockSpec(memory_space=pltpu.VMEM)
    hbm = pl.BlockSpec(memory_space=pltpu.HBM)
    smem = pl.BlockSpec(memory_space=pltpu.SMEM)
    bf16 = jnp.bfloat16
    return pl.pallas_call(
        functools.partial(kernel, parts, groups, pieces, widths),
        out_shape=pltpu.VMEM((owned, out_cols), bf16),
        in_specs=[hbm] * 3 + [smem] + [hbm] * 7,
        out_specs=vmem,
        scratch_shapes=[
            pltpu.VMEM((block_count + parts * slots, w, BLOCK), bf16) for w in widths
        ] + [
            pltpu.VMEM((block_count, w, BLOCK), bf16) for w in widths
        ] + [
            pltpu.VMEM((parts, slots, w, BLOCK), bf16) for w in widths
        ] + [
            pltpu.VMEM((w, rows), bf16) for w in widths
        ] + [
            pltpu.SMEM(send_blocks.shape, jnp.int32),
            pltpu.SMEM(counts.shape, jnp.int32),
            pltpu.SMEM(tile_blocks.shape, jnp.int32),
            pltpu.VMEM((block_count, BLOCK), jnp.int32),
            pltpu.VMEM((1, hidden_cols), jnp.float32),
            pltpu.VMEM((1, out_cols), jnp.float32),
            pltpu.VMEM(neighbours.shape, jnp.int32),
            pltpu.VMEM((depth, hidden_cols), bf16),
            pltpu.VMEM((hidden_cols, out_cols), bf16),
            pltpu.VMEM((pieces, groups, cols, owned // pieces), bf16),
            pltpu.VMEM((pieces, groups, cols, owned // pieces), bf16),
            pltpu.SemaphoreType.DMA((1,)),
            pltpu.SemaphoreType.DMA((chunks,)),
            pltpu.SemaphoreType.DMA((1,)),
            pltpu.SemaphoreType.DMA((pieces,)),
            pltpu.SemaphoreType.DMA((chunks + 3,)),
        ],
        compiler_params=pltpu.CompilerParams(
            collective_id=0, has_side_effects=True, vmem_limit_bytes=56 * 1024 * 1024
        ),
    )(
        send_blocks, counts, tile_blocks, epsilon,
        degree.reshape(block_count, BLOCK), b_first.reshape(1, -1), b_second.reshape(1, -1),
        features, neighbours, w_first, w_second,
    )


def solution(mesh):
    return jax.shard_map(
        per_device,
        mesh=mesh,
        in_specs=(
            P("feat", "dom"),
            P("dom", None, None),
            P("dom", None),
            P(None, "dom"),
            P(None, "dom"),
            P("dom"),
            P(), P(), P(), P(), P(),
        ),
        out_specs=P(("dom", "feat"), None),
        check_vma=False,
    )
```

```python
import functools

import jax
import jax.numpy as jnp
from jax import lax
from jax.experimental import pallas as pl
from jax.experimental.pallas import tpu as pltpu
from jax.sharding import PartitionSpec as P

BLOCK = 128
SUBLANES = 16
SPLITS = 2
RAW = 8
PIECES = 4


def chunk_widths(cols):
    widths = []
    while sum(widths) < cols:
        widths.append(min(max(SUBLANES, sum(widths)), cols - sum(widths)))
    return widths


def kernel(
    parts, groups, pieces, widths,
    sb_hbm, cnt_hbm, tile_hbm, eps_ref, deg_hbm, b1_hbm, b2_hbm,
    feat_hbm, nbr_hbm, w1_hbm, w2_hbm,
    out_ref, parcel, w1_ref, w2_ref, b1_ref, b2_ref,
    *scratch,
):
    chunks = len(widths) - 1
    swap = chunks
    starts = [sum(widths[:c]) for c in range(chunks)]
    raw_start = sum(widths[:chunks])
    cols = raw_start + RAW
    count = len(widths)
    tables, locals_, stages, feats = (scratch[i * count:(i + 1) * count] for i in range(4))
    (sb_ref, cnt_ref, tile_ref, deg_ref, nbr_ref, zstage, zswap,
     hsend, hrecv, zsend, zrecv, zlast, raw_sem, in_sem) = scratch[4 * count:]
    me = lax.axis_index("dom")
    z = lax.axis_index("feat")
    slots = stages[0].shape[1]
    list_width, block_count = tile_ref.shape
    per_piece = block_count // groups // pieces
    piece_nodes = per_piece * BLOCK
    splits = zlast.shape[1]
    part_blocks = per_piece // splits
    part_nodes = part_blocks * BLOCK
    last = chunks - 1
    half = groups // 2
    partner = lax.rem(z + half, groups)

    def lanes(block):
        return pl.ds(pl.multiple_of(block * BLOCK, BLOCK), BLOCK)

    def halo_copy(c, peer, source):
        return pltpu.make_async_remote_copy(
            src_ref=stages[c].at[peer],
            dst_ref=tables[c].at[pl.ds(block_count + source * slots, slots)],
            send_sem=hsend.at[0],
            recv_sem=hrecv.at[c],
            device_id={"dom": peer},
            device_id_type=pl.DeviceIdType.MESH,
        )

    def parcel_rows(source, start, size):
        return pl.ds(pl.multiple_of(source * cols + start, RAW), size)

    def row_copy(c, p, dest):
        return pltpu.make_async_remote_copy(
            src_ref=zstage.at[p, dest, pl.ds(starts[c], widths[c])],
            dst_ref=parcel.at[p, parcel_rows(z, starts[c], widths[c])],
            send_sem=zsend.at[0],
            recv_sem=zrecv.at[p],
            device_id={"feat": dest},
            device_id_type=pl.DeviceIdType.MESH,
        )

    def part_lanes(h):
        return pl.ds(pl.multiple_of(h * part_nodes, BLOCK), part_nodes)

    def last_copy(p, h, dest):
        rows = pl.ds(starts[last], widths[last])
        return pltpu.make_async_remote_copy(
            src_ref=zstage.at[p, dest, rows, part_lanes(h)],
            dst_ref=parcel.at[p, parcel_rows(z, starts[last], widths[last]), part_lanes(h)],
            send_sem=zsend.at[0],
            recv_sem=zlast.at[p, h],
            device_id={"feat": dest},
            device_id_type=pl.DeviceIdType.MESH,
        )

    def swap_copy(p, i, part, owner):
        return pltpu.make_async_remote_copy(
            src_ref=zswap.at[p, i, pl.ds(part * RAW, RAW)],
            dst_ref=parcel.at[p, parcel_rows(owner, raw_start, RAW)],
            send_sem=zsend.at[0],
            recv_sem=zrecv.at[p],
            device_id={"feat": sibling(i)},
            device_id_type=pl.DeviceIdType.MESH,
        )

    def raw_copy():
        return pltpu.make_async_remote_copy(
            src_ref=feats[swap].at[pl.ds(0, RAW)],
            dst_ref=feats[swap].at[pl.ds(RAW, RAW)],
            send_sem=raw_sem.at[0],
            recv_sem=raw_sem.at[1],
            device_id={"feat": partner},
            device_id_type=pl.DeviceIdType.MESH,
        )

    def halo_all(c, sem):
        blocks = tables[c].at[pl.ds(0, (parts - 1) * slots)]
        return pltpu.make_async_copy(blocks, blocks, sem)

    def row_all(p, sem, dropped=0):
        rows = parcel.at[p, pl.ds(0, (groups - 1) * (cols - dropped) - RAW)]
        return pltpu.make_async_copy(rows, rows, sem)

    def last_all(p, h):
        rows = parcel.at[p, pl.ds(0, (groups - 1) * widths[last]), part_lanes(h)]
        return pltpu.make_async_copy(rows, rows, zlast.at[p, h])

    def sibling(i):
        return (z // half) * half + lax.rem(lax.rem(z, half) + i, half)

    def dest_of(k):
        if k < half:
            lower = z // half
            return lower * k + (1 - lower) * (groups - 1 - k)
        return sibling(k - half + 1)

    barrier = pltpu.get_barrier_semaphore()

    @pl.loop(1, groups)
    def _(k):
        pl.semaphore_signal(
            barrier, inc=1, device_id={"feat": lax.rem(z + k, groups)},
            device_id_type=pl.DeviceIdType.MESH,
        )

    @pl.loop(1, parts)
    def _(k):
        pl.semaphore_signal(
            barrier, inc=1, device_id={"dom": lax.rem(me + k, parts)},
            device_id_type=pl.DeviceIdType.MESH,
        )

    loads = [
        pltpu.make_async_copy(
            feat_hbm.at[pl.ds(starts[c], widths[c])], feats[c], in_sem.at[c]
        )
        for c in range(chunks)
    ]
    raw_load = pltpu.make_async_copy(
        feat_hbm.at[pl.ds(raw_start, RAW)], feats[swap].at[pl.ds(0, RAW)], in_sem.at[swap]
    )
    small = [
        pltpu.make_async_copy(source, target, in_sem.at[count])
        for source, target in ((sb_hbm, sb_ref), (cnt_hbm, cnt_ref))
    ]
    lists = [
        pltpu.make_async_copy(source, target, in_sem.at[count + 1])
        for source, target in ((tile_hbm, tile_ref), (deg_hbm, deg_ref), (nbr_hbm, nbr_ref))
    ]
    weights = [
        pltpu.make_async_copy(source, target, in_sem.at[count + 2])
        for source, target in (
            (w1_hbm, w1_ref), (w2_hbm, w2_ref), (b1_hbm, b1_ref), (b2_hbm, b2_ref),
        )
    ]
    for load in loads[:1] + small + [raw_load] + loads[1:] + lists + weights:
        load.start()

    def lay_out(c):
        @pl.loop(0, block_count, unroll=4)
        def _(b):
            block = feats[c][:, lanes(b)]
            locals_[c][b] = block
            tables[c][b] = block

        tables[c][pl.ds(block_count + me * slots, slots)] = jnp.zeros(
            (slots, widths[c], BLOCK), jnp.bfloat16
        )

    def fill(c, peer):
        for s in range(slots):
            used = (s < cnt_ref[0, peer]).astype(jnp.float32)
            block = locals_[c][sb_ref[0, peer, s]]
            stages[c][peer, s] = (block.astype(jnp.float32) * used).astype(jnp.bfloat16)

    def send_halo(c):
        @pl.loop(1, parts)
        def _(k):
            peer = lax.rem(me + k, parts)
            fill(c, peer)
            halo_copy(c, peer, me).start()

    loads[0].wait()
    lay_out(0)
    for load in small:
        load.wait()

    @pl.loop(1, parts)
    def _(k):
        fill(0, lax.rem(me + k, parts))

    raw_load.wait()
    pl.semaphore_wait(barrier, parts + groups - 2)

    raw_copy().start()

    @pl.loop(1, parts)
    def _(k):
        halo_copy(0, lax.rem(me + k, parts), me).start()

    for c in range(1, chunks):
        loads[c].wait()
        lay_out(c)
        send_halo(c)

    for load in lists:
        load.wait()
    gain = 1.0 + eps_ref[0]

    lane_gather = lax.GatherDimensionNumbers(
        offset_dims=(), collapsed_slice_dims=(1,), start_index_map=(1,),
        operand_batching_dims=(0,), start_indices_batching_dims=(0,),
    )

    def mixed_block(c, b):
        shape = (widths[c], BLOCK)
        total = gain * feats[c][:, lanes(b)].astype(jnp.float32)
        near = jnp.zeros(shape, jnp.float32)
        degree = jnp.broadcast_to(deg_ref[pl.ds(b, 1), :], shape)
        for j in range(list_width):
            tile = tables[c][tile_ref[j, b]].astype(jnp.float32)
            index = jnp.broadcast_to(nbr_ref[pl.ds(j, 1), lanes(b)], shape)
            taken = lax.gather(
                tile, index[..., None], lane_gather, slice_sizes=(1, 1),
                mode=lax.GatherScatterMode.PROMISE_IN_BOUNDS,
            )
            near = near + jnp.where(degree > j, taken, 0.0)
        return (total + near).astype(jnp.bfloat16)

    def blocks_of(c, p, dest, store):
        first = (dest * pieces + p) * per_piece
        unroll = per_piece if widths[c] <= 2 * SUBLANES else max(per_piece // 2, 1)

        @pl.loop(0, per_piece, unroll=unroll)
        def _(i):
            store(i, mixed_block(c, first + i))

    def aggregate(c, p, k):
        dest = dest_of(k) if k < groups - 1 else z

        def store(i, block):
            if k < groups - 1:
                zstage[p, dest, pl.ds(starts[c], widths[c]), lanes(i)] = block
            else:
                parcel[p, parcel_rows(z, starts[c], widths[c]), lanes(i)] = block

        blocks_of(c, p, dest, store)
        if k < groups - 1:
            row_copy(c, p, dest).start()

    def aggregate_swap(p, i):
        def store(n, block):
            if i > 0:
                zswap[p, i, :, lanes(n)] = block
            else:
                parcel[p, parcel_rows(z, raw_start, RAW), lanes(n)] = block[:RAW]
                parcel[p, parcel_rows(partner, raw_start, RAW), lanes(n)] = block[RAW:]

        blocks_of(swap, p, sibling(i), store)
        if i > 0:
            swap_copy(p, i, 0, z).start()
            swap_copy(p, i, 1, partner).start()

    def aggregate_last(p, k):
        dest = dest_of(k) if k < groups - 1 else z
        first = (dest * pieces + p) * per_piece
        rows = pl.ds(starts[last], widths[last])

        @pl.loop(0, splits)
        def _(h):
            for n in range(part_blocks):
                i = h * part_blocks + n
                block = mixed_block(last, first + i)
                if k < groups - 1:
                    zstage[p, dest, rows, lanes(i)] = block
                else:
                    parcel[p, parcel_rows(z, starts[last], widths[last]), lanes(i)] = block
            if k < groups - 1:
                last_copy(p, h, dest).start()

    def run(c, ks):
        @pl.loop(0, pieces)
        def _(p):
            for k in ks:
                aggregate(c, p, k)

    def run_ending(ks):
        for k in ks:
            @pl.loop(pieces - ending, pieces)
            def _(p):
                aggregate_last(p, k)

    across, within = range(half), range(half, groups)
    ending = pieces // 2
    for c in range(chunks):
        halo_all(c, hrecv.at[c]).wait()
        if c == chunks - 1:
            halo_all(swap, hrecv.at[swap]).wait()

            @pl.loop(0, pieces - ending)
            def _(p):
                for k in range(groups):
                    aggregate_last(p, k)
                for i in reversed(range(half)):
                    aggregate_swap(p, i)

            run_ending(across[:half // 2])

            @pl.loop(pieces - ending, pieces)
            def _(p):
                for k in within[:-1]:
                    aggregate_last(p, k)
                for i in reversed(range(half)):
                    aggregate_swap(p, i)

            run_ending(across[half // 2:])
            run_ending(within[-1:])
        else:
            run(c, across)
        if c == min(1, chunks - 2):
            raw_copy().wait()
            lay_out(swap)
            send_halo(swap)
        if 0 < c < chunks - 1:
            run(c - 1, within)
        if c == chunks - 2:
            run(c, within)

    for load in weights:
        load.wait()
    for c in range(count):
        halo_all(c, hsend.at[0]).wait()

    def finish(p, h):
        last_all(p, h).wait()
        first = pl.multiple_of((p * splits + h) * part_nodes, part_nodes)
        out_ref[pl.ds(first, part_nodes), :] = network(
            parcel[p, :, part_lanes(h)], w1_ref, w2_ref, b1_ref, b2_ref
        )

    @pl.loop(0, pieces - 1)
    def _(p):
        row_all(p, zrecv.at[p], widths[last]).wait()

        @pl.loop(0, splits)
        def _(h):
            finish(p, h)

    final = pieces - 1
    row_all(final, zrecv.at[final], widths[last]).wait()
    for p in range(final):
        row_all(p, zsend.at[0]).wait()
    for h in range(splits - 1):
        finish(final, h)
    last_all(final, splits - 1).wait()
    row_all(final, zsend.at[0]).wait()


def network(columns, w1_ref, w2_ref, b1_ref, b2_ref):
    hidden = lax.dot_general(
        columns, w1_ref[...], (((0,), (0,)), ((), ())), preferred_element_type=jnp.float32
    ) + b1_ref[...]
    hidden = jnp.maximum(hidden, 0.0).astype(jnp.bfloat16)
    return (
        jnp.dot(hidden, w2_ref[...], preferred_element_type=jnp.float32) + b2_ref[...]
    ).astype(jnp.bfloat16)


def closing_kernel(
    part_nodes, out_ref, parcel, w1_ref, w2_ref, b1_ref, b2_ref, result_hbm, rest_ref, sems
):
    done = out_ref.shape[0] - part_nodes
    pieces, _, piece_nodes = parcel.shape
    early = pltpu.make_async_copy(
        out_ref.at[pl.ds(0, done)], result_hbm.at[pl.ds(0, done)], sems.at[0]
    )
    early.start()
    columns = parcel[pieces - 1, :, pl.ds(piece_nodes - part_nodes, part_nodes)]
    rest_ref[...] = network(columns, w1_ref, w2_ref, b1_ref, b2_ref)
    late = pltpu.make_async_copy(
        rest_ref, result_hbm.at[pl.ds(done, part_nodes)], sems.at[1]
    )
    late.start()
    early.wait()
    late.wait()


def in_hbm(array):
    return pltpu.with_memory_space_constraint(array, pltpu.HBM)


def per_device(
    features, send_blocks, counts, tile_blocks, neighbours, degree, epsilon,
    w_first, b_first, w_second, b_second,
):
    parts = lax.axis_size("dom")
    groups = lax.axis_size("feat")
    cols, rows = features.shape
    slots = send_blocks.shape[2]
    widths = chunk_widths(cols - RAW) + [2 * RAW]
    count = len(widths)
    block_count = rows // BLOCK
    owned = rows // groups
    pieces = min(PIECES, owned // BLOCK)
    splits = SPLITS if (owned // BLOCK // pieces) % SPLITS == 0 else 1
    hidden_cols, out_cols = w_second.shape
    depth = w_first.shape[0]
    hbm = pl.BlockSpec(memory_space=pltpu.HBM)
    smem = pl.BlockSpec(memory_space=pltpu.SMEM)
    bf16 = jnp.bfloat16
    vmem = pl.BlockSpec(memory_space=pltpu.VMEM)
    part_nodes = owned // pieces // splits
    handed = pl.pallas_call(
        functools.partial(kernel, parts, groups, pieces, widths),
        out_shape=(
            pltpu.VMEM((owned, out_cols), bf16),
            pltpu.VMEM((pieces, depth, owned // pieces), bf16),
            pltpu.VMEM((depth, hidden_cols), bf16),
            pltpu.VMEM((hidden_cols, out_cols), bf16),
            pltpu.VMEM((1, hidden_cols), jnp.float32),
            pltpu.VMEM((1, out_cols), jnp.float32),
        ),
        in_specs=[hbm] * 3 + [smem] + [hbm] * 7,
        out_specs=(vmem,) * 6,
        scratch_shapes=[
            pltpu.VMEM((block_count + parts * slots, w, BLOCK), bf16) for w in widths
        ] + [
            pltpu.VMEM((block_count, w, BLOCK), bf16) for w in widths
        ] + [
            pltpu.VMEM((parts, slots, w, BLOCK), bf16) for w in widths
        ] + [
            pltpu.VMEM((w, rows), bf16) for w in widths
        ] + [
            pltpu.SMEM(send_blocks.shape, jnp.int32),
            pltpu.SMEM(counts.shape, jnp.int32),
            pltpu.SMEM(tile_blocks.shape, jnp.int32),
            pltpu.VMEM((block_count, BLOCK), jnp.int32),
            pltpu.VMEM(neighbours.shape, jnp.int32),
            pltpu.VMEM((pieces, groups, cols, owned // pieces), bf16),
            pltpu.VMEM((pieces, groups // 2, 2 * RAW, owned // pieces), bf16),
            pltpu.SemaphoreType.DMA((1,)),
            pltpu.SemaphoreType.DMA((count,)),
            pltpu.SemaphoreType.DMA((1,)),
            pltpu.SemaphoreType.DMA((pieces,)),
            pltpu.SemaphoreType.DMA((pieces, splits)),
            pltpu.SemaphoreType.DMA((2,)),
            pltpu.SemaphoreType.DMA((count + 3,)),
        ],
        compiler_params=pltpu.CompilerParams(
            collective_id=0, has_side_effects=True, vmem_limit_bytes=48 * 1024 * 1024
        ),
    )(
        in_hbm(send_blocks), in_hbm(counts), in_hbm(tile_blocks), epsilon,
        in_hbm(degree.reshape(block_count, BLOCK)),
        in_hbm(b_first.reshape(1, -1)), in_hbm(b_second.reshape(1, -1)),
        in_hbm(features), in_hbm(neighbours), in_hbm(w_first), in_hbm(w_second),
    )
    return pl.pallas_call(
        functools.partial(closing_kernel, part_nodes),
        out_shape=jax.ShapeDtypeStruct((owned, out_cols), bf16),
        in_specs=[vmem] * 6,
        out_specs=hbm,
        scratch_shapes=[
            pltpu.VMEM((part_nodes, out_cols), bf16), pltpu.SemaphoreType.DMA((2,)),
        ],
        compiler_params=pltpu.CompilerParams(vmem_limit_bytes=16 * 1024 * 1024),
    )(*handed)


def solution(mesh):
    return jax.shard_map(
        per_device,
        mesh=mesh,
        in_specs=(
            P("feat", "dom"),
            P("dom", None, None),
            P("dom", None),
            P(None, "dom"),
            P(None, "dom"),
            P("dom"),
            P(), P(), P(), P(), P(),
        ),
        out_specs=P(("dom", "feat"), None),
        check_vma=False,
    )
```

```python
import functools

import jax
import jax.numpy as jnp
from jax import lax
from jax.experimental import pallas as pl
from jax.experimental.pallas import tpu as pltpu
from jax.sharding import PartitionSpec as P

BLOCK = 128
SUBLANES = 16
SPLITS = 2
RAW = 8
PIECES = 4


def chunk_widths(cols):
    widths = []
    while sum(widths) < cols:
        widths.append(min(max(SUBLANES, sum(widths)), cols - sum(widths)))
    return widths


def kernel(
    parts, groups, pieces, widths,
    sb_hbm, cnt_hbm, tile_hbm, eps_ref, deg_hbm, b1_hbm, b2_hbm,
    feat_hbm, nbr_hbm, w1_hbm, w2_hbm,
    out_ref, parcel, w1_ref, w2_ref, b1_ref, b2_ref,
    *scratch,
):
    chunks = len(widths) - 1
    swap = chunks
    starts = [sum(widths[:c]) for c in range(chunks)]
    raw_start = sum(widths[:chunks])
    cols = raw_start + RAW
    count = len(widths)
    tables, locals_, stages, feats = (scratch[i * count:(i + 1) * count] for i in range(4))
    (sb_ref, cnt_ref, tile_ref, deg_ref, nbr_ref, zstage, zswap,
     hsend, hrecv, zsend, zrecv, zlast, raw_sem, in_sem) = scratch[4 * count:]
    me = lax.axis_index("dom")
    z = lax.axis_index("feat")
    slots = stages[0].shape[1]
    list_width, block_count = tile_ref.shape
    per_piece = block_count // groups // pieces
    piece_nodes = per_piece * BLOCK
    splits = zlast.shape[1]
    part_blocks = per_piece // splits
    part_nodes = part_blocks * BLOCK
    last = chunks - 1
    half = groups // 2
    partner = groups - 1 - z

    def lanes(block):
        return pl.ds(pl.multiple_of(block * BLOCK, BLOCK), BLOCK)

    def halo_copy(c, peer, source):
        return pltpu.make_async_remote_copy(
            src_ref=stages[c].at[peer],
            dst_ref=tables[c].at[pl.ds(block_count + source * slots, slots)],
            send_sem=hsend.at[0],
            recv_sem=hrecv.at[c],
            device_id={"dom": peer},
            device_id_type=pl.DeviceIdType.MESH,
        )

    def parcel_rows(source, start, size):
        return pl.ds(pl.multiple_of(source * cols + start, RAW), size)

    def row_copy(c, p, dest):
        return pltpu.make_async_remote_copy(
            src_ref=zstage.at[p, dest, pl.ds(starts[c], widths[c])],
            dst_ref=parcel.at[p, parcel_rows(z, starts[c], widths[c])],
            send_sem=zsend.at[0],
            recv_sem=zrecv.at[p],
            device_id={"feat": dest},
            device_id_type=pl.DeviceIdType.MESH,
        )

    def part_lanes(h):
        return pl.ds(pl.multiple_of(h * part_nodes, BLOCK), part_nodes)

    def last_copy(p, h, dest):
        rows = pl.ds(starts[last], widths[last])
        return pltpu.make_async_remote_copy(
            src_ref=zstage.at[p, dest, rows, part_lanes(h)],
            dst_ref=parcel.at[p, parcel_rows(z, starts[last], widths[last]), part_lanes(h)],
            send_sem=zsend.at[0],
            recv_sem=zlast.at[p, h],
            device_id={"feat": dest},
            device_id_type=pl.DeviceIdType.MESH,
        )

    def swap_copy(p, i, part, owner):
        return pltpu.make_async_remote_copy(
            src_ref=zswap.at[p, i, pl.ds(part * RAW, RAW)],
            dst_ref=parcel.at[p, parcel_rows(owner, raw_start, RAW)],
            send_sem=zsend.at[0],
            recv_sem=zrecv.at[p],
            device_id={"feat": sibling(i)},
            device_id_type=pl.DeviceIdType.MESH,
        )

    def raw_copy():
        return pltpu.make_async_remote_copy(
            src_ref=feats[swap].at[pl.ds(0, RAW)],
            dst_ref=feats[swap].at[pl.ds(RAW, RAW)],
            send_sem=raw_sem.at[0],
            recv_sem=raw_sem.at[1],
            device_id={"feat": partner},
            device_id_type=pl.DeviceIdType.MESH,
        )

    def halo_all(c, sem):
        blocks = tables[c].at[pl.ds(0, (parts - 1) * slots)]
        return pltpu.make_async_copy(blocks, blocks, sem)

    def row_all(p, sem, dropped=0):
        rows = parcel.at[p, pl.ds(0, (groups - 1) * (cols - dropped) - RAW)]
        return pltpu.make_async_copy(rows, rows, sem)

    def last_all(p, h):
        rows = parcel.at[p, pl.ds(0, (groups - 1) * widths[last]), part_lanes(h)]
        return pltpu.make_async_copy(rows, rows, zlast.at[p, h])

    def sibling(i):
        return (z // half) * half + lax.rem(lax.rem(z, half) + i, half)

    def dest_of(k):
        if k < half:
            lower = z // half
            return lower * k + (1 - lower) * (groups - 1 - k)
        return sibling(k - half + 1)

    def peer_of(k):
        peer, bit = 0, 1
        while bit < parts:
            peer = peer + lax.rem(me // bit + k // bit, 2) * bit
            bit *= 2
        return peer

    barrier = pltpu.get_barrier_semaphore()

    for k in range(1, groups):
        pl.semaphore_signal(
            barrier, inc=1, device_id={"feat": lax.rem(z + k, groups)},
            device_id_type=pl.DeviceIdType.MESH,
        )
    for k in reversed(range(1, parts)):
        pl.semaphore_signal(
            barrier, inc=1, device_id={"dom": peer_of(k)},
            device_id_type=pl.DeviceIdType.MESH,
        )

    loads = [
        pltpu.make_async_copy(
            feat_hbm.at[pl.ds(starts[c], widths[c])], feats[c], in_sem.at[c]
        )
        for c in range(chunks)
    ]
    raw_load = pltpu.make_async_copy(
        feat_hbm.at[pl.ds(raw_start, RAW)], feats[swap].at[pl.ds(0, RAW)], in_sem.at[swap]
    )
    small = [
        pltpu.make_async_copy(source, target, in_sem.at[count])
        for source, target in ((sb_hbm, sb_ref), (cnt_hbm, cnt_ref))
    ]
    lists = [
        pltpu.make_async_copy(source, target, in_sem.at[count + 1])
        for source, target in ((tile_hbm, tile_ref), (deg_hbm, deg_ref), (nbr_hbm, nbr_ref))
    ]
    weights = [
        pltpu.make_async_copy(source, target, in_sem.at[count + 2])
        for source, target in (
            (w1_hbm, w1_ref), (w2_hbm, w2_ref), (b1_hbm, b1_ref), (b2_hbm, b2_ref),
        )
    ]
    for load in loads[:1] + small + [raw_load] + loads[1:] + lists + weights:
        load.start()

    def lay_out(c):
        @pl.loop(0, block_count, unroll=4)
        def _(b):
            block = feats[c][:, lanes(b)]
            locals_[c][b] = block
            tables[c][b] = block

        tables[c][pl.ds(block_count + me * slots, slots)] = jnp.zeros(
            (slots, widths[c], BLOCK), jnp.bfloat16
        )

    def fill(c, peer):
        for s in range(slots):
            used = (s < cnt_ref[0, peer]).astype(jnp.float32)
            block = locals_[c][sb_ref[0, peer, s]]
            stages[c][peer, s] = (block.astype(jnp.float32) * used).astype(jnp.bfloat16)

    def send_halo(c):
        @pl.loop(1, parts)
        def _(k):
            peer = peer_of(parts - k)
            fill(c, peer)
            halo_copy(c, peer, me).start()

    loads[0].wait()
    lay_out(0)
    for load in small:
        load.wait()

    @pl.loop(1, parts)
    def _(k):
        fill(0, lax.rem(me + k, parts))

    raw_load.wait()
    pl.semaphore_wait(barrier, parts + groups - 2)

    raw_copy().start()

    for k in reversed(range(1, parts)):
        halo_copy(0, peer_of(k), me).start()

    for c in range(1, chunks):
        loads[c].wait()
        lay_out(c)
        send_halo(c)

    for load in lists:
        load.wait()
    gain = 1.0 + eps_ref[0]

    lane_gather = lax.GatherDimensionNumbers(
        offset_dims=(), collapsed_slice_dims=(1,), start_index_map=(1,),
        operand_batching_dims=(0,), start_indices_batching_dims=(0,),
    )

    def mixed_block(c, b):
        shape = (widths[c], BLOCK)
        total = gain * feats[c][:, lanes(b)].astype(jnp.float32)
        near = jnp.zeros(shape, jnp.float32)
        degree = jnp.broadcast_to(deg_ref[pl.ds(b, 1), :], shape)
        for j in range(list_width):
            tile = tables[c][tile_ref[j, b]].astype(jnp.float32)
            index = jnp.broadcast_to(nbr_ref[pl.ds(j, 1), lanes(b)], shape)
            taken = lax.gather(
                tile, index[..., None], lane_gather, slice_sizes=(1, 1),
                mode=lax.GatherScatterMode.PROMISE_IN_BOUNDS,
            )
            near = near + jnp.where(degree > j, taken, 0.0)
        return (total + near).astype(jnp.bfloat16)

    def blocks_of(c, p, dest, store):
        first = (dest * pieces + p) * per_piece
        unroll = per_piece if widths[c] <= 2 * SUBLANES else max(per_piece // 2, 1)

        @pl.loop(0, per_piece, unroll=unroll)
        def _(i):
            store(i, mixed_block(c, first + i))

    def aggregate(c, p, k):
        dest = dest_of(k) if k < groups - 1 else z

        def store(i, block):
            if k < groups - 1:
                zstage[p, dest, pl.ds(starts[c], widths[c]), lanes(i)] = block
            else:
                parcel[p, parcel_rows(z, starts[c], widths[c]), lanes(i)] = block

        blocks_of(c, p, dest, store)
        if k < groups - 1:
            row_copy(c, p, dest).start()

    def aggregate_swap(p, i):
        def store(n, block):
            if i > 0:
                zswap[p, i, :, lanes(n)] = block
            else:
                parcel[p, parcel_rows(z, raw_start, RAW), lanes(n)] = block[:RAW]
                parcel[p, parcel_rows(partner, raw_start, RAW), lanes(n)] = block[RAW:]

        blocks_of(swap, p, sibling(i), store)
        if i > 0:
            swap_copy(p, i, 0, z).start()
            swap_copy(p, i, 1, partner).start()

    def aggregate_last(p, k):
        dest = dest_of(k) if k < groups - 1 else z
        first = (dest * pieces + p) * per_piece
        rows = pl.ds(starts[last], widths[last])

        @pl.loop(0, splits)
        def _(h):
            for n in range(part_blocks):
                i = h * part_blocks + n
                block = mixed_block(last, first + i)
                if k < groups - 1:
                    zstage[p, dest, rows, lanes(i)] = block
                else:
                    parcel[p, parcel_rows(z, starts[last], widths[last]), lanes(i)] = block
            if k < groups - 1:
                last_copy(p, h, dest).start()

    def run(c, ks):
        @pl.loop(0, pieces)
        def _(p):
            for k in ks:
                aggregate(c, p, k)

    def run_ending(ks):
        for k in ks:
            @pl.loop(pieces - ending, pieces)
            def _(p):
                aggregate_last(p, k)

    across, within = range(half), range(half, groups)
    ending = pieces // 2
    for c in range(chunks):
        halo_all(c, hrecv.at[c]).wait()
        if c == chunks - 1:
            halo_all(swap, hrecv.at[swap]).wait()

            @pl.loop(0, pieces - ending)
            def _(p):
                for k in range(groups):
                    aggregate_last(p, k)
                for i in reversed(range(half)):
                    aggregate_swap(p, i)

            run_ending(across[:half // 2])

            @pl.loop(pieces - ending, pieces)
            def _(p):
                for k in within[:-1]:
                    aggregate_last(p, k)
                for i in reversed(range(half)):
                    aggregate_swap(p, i)

            run_ending(across[half // 2:])
            run_ending(within[-1:])
        else:
            run(c, across)
        if c == min(1, chunks - 2):
            raw_copy().wait()
            lay_out(swap)
            send_halo(swap)
        if 0 < c < chunks - 1:
            run(c - 1, within)
        if c == chunks - 2:
            run(c, within)

    for load in weights:
        load.wait()
    for c in range(count):
        halo_all(c, hsend.at[0]).wait()

    def finish(p, h):
        last_all(p, h).wait()
        first = pl.multiple_of((p * splits + h) * part_nodes, part_nodes)
        out_ref[pl.ds(first, part_nodes), :] = network(
            parcel[p, :, part_lanes(h)], w1_ref, w2_ref, b1_ref, b2_ref
        )

    @pl.loop(0, pieces - 1)
    def _(p):
        row_all(p, zrecv.at[p], widths[last]).wait()

        @pl.loop(0, splits)
        def _(h):
            finish(p, h)

    final = pieces - 1
    row_all(final, zrecv.at[final], widths[last]).wait()
    for p in range(final):
        row_all(p, zsend.at[0]).wait()
    for h in range(splits - 1):
        finish(final, h)
    last_all(final, splits - 1).wait()
    row_all(final, zsend.at[0]).wait()


def network(columns, w1_ref, w2_ref, b1_ref, b2_ref):
    hidden = lax.dot_general(
        columns, w1_ref[...], (((0,), (0,)), ((), ())), preferred_element_type=jnp.float32
    ) + b1_ref[...]
    hidden = jnp.maximum(hidden, 0.0).astype(jnp.bfloat16)
    return (
        jnp.dot(hidden, w2_ref[...], preferred_element_type=jnp.float32) + b2_ref[...]
    ).astype(jnp.bfloat16)


def closing_kernel(
    part_nodes, out_ref, parcel, w1_ref, w2_ref, b1_ref, b2_ref, result_hbm, rest_ref, sems
):
    done = out_ref.shape[0] - part_nodes
    pieces, _, piece_nodes = parcel.shape
    early = pltpu.make_async_copy(
        out_ref.at[pl.ds(0, done)], result_hbm.at[pl.ds(0, done)], sems.at[0]
    )
    early.start()
    columns = parcel[pieces - 1, :, pl.ds(piece_nodes - part_nodes, part_nodes)]
    rest_ref[...] = network(columns, w1_ref, w2_ref, b1_ref, b2_ref)
    late = pltpu.make_async_copy(
        rest_ref, result_hbm.at[pl.ds(done, part_nodes)], sems.at[1]
    )
    late.start()
    early.wait()
    late.wait()


def in_hbm(array):
    return pltpu.with_memory_space_constraint(array, pltpu.HBM)


def per_device(
    features, send_blocks, counts, tile_blocks, neighbours, degree, epsilon,
    w_first, b_first, w_second, b_second,
):
    parts = lax.axis_size("dom")
    groups = lax.axis_size("feat")
    cols, rows = features.shape
    slots = send_blocks.shape[2]
    widths = chunk_widths(cols - RAW) + [2 * RAW]
    count = len(widths)
    block_count = rows // BLOCK
    owned = rows // groups
    pieces = min(PIECES, owned // BLOCK)
    splits = SPLITS if (owned // BLOCK // pieces) % SPLITS == 0 else 1
    hidden_cols, out_cols = w_second.shape
    depth = w_first.shape[0]
    hbm = pl.BlockSpec(memory_space=pltpu.HBM)
    smem = pl.BlockSpec(memory_space=pltpu.SMEM)
    bf16 = jnp.bfloat16
    vmem = pl.BlockSpec(memory_space=pltpu.VMEM)
    part_nodes = owned // pieces // splits
    handed = pl.pallas_call(
        functools.partial(kernel, parts, groups, pieces, widths),
        out_shape=(
            pltpu.VMEM((owned, out_cols), bf16),
            pltpu.VMEM((pieces, depth, owned // pieces), bf16),
            pltpu.VMEM((depth, hidden_cols), bf16),
            pltpu.VMEM((hidden_cols, out_cols), bf16),
            pltpu.VMEM((1, hidden_cols), jnp.float32),
            pltpu.VMEM((1, out_cols), jnp.float32),
        ),
        in_specs=[hbm] * 3 + [smem] + [hbm] * 7,
        out_specs=(vmem,) * 6,
        scratch_shapes=[
            pltpu.VMEM((block_count + parts * slots, w, BLOCK), bf16) for w in widths
        ] + [
            pltpu.VMEM((block_count, w, BLOCK), bf16) for w in widths
        ] + [
            pltpu.VMEM((parts, slots, w, BLOCK), bf16) for w in widths
        ] + [
            pltpu.VMEM((w, rows), bf16) for w in widths
        ] + [
            pltpu.SMEM(send_blocks.shape, jnp.int32),
            pltpu.SMEM(counts.shape, jnp.int32),
            pltpu.SMEM(tile_blocks.shape, jnp.int32),
            pltpu.VMEM((block_count, BLOCK), jnp.int32),
            pltpu.VMEM(neighbours.shape, jnp.int32),
            pltpu.VMEM((pieces, groups, cols, owned // pieces), bf16),
            pltpu.VMEM((pieces, groups // 2, 2 * RAW, owned // pieces), bf16),
            pltpu.SemaphoreType.DMA((1,)),
            pltpu.SemaphoreType.DMA((count,)),
            pltpu.SemaphoreType.DMA((1,)),
            pltpu.SemaphoreType.DMA((pieces,)),
            pltpu.SemaphoreType.DMA((pieces, splits)),
            pltpu.SemaphoreType.DMA((2,)),
            pltpu.SemaphoreType.DMA((count + 3,)),
        ],
        compiler_params=pltpu.CompilerParams(
            collective_id=0, has_side_effects=True, vmem_limit_bytes=48 * 1024 * 1024
        ),
    )(
        in_hbm(send_blocks), in_hbm(counts), in_hbm(tile_blocks), epsilon,
        in_hbm(degree.reshape(block_count, BLOCK)),
        in_hbm(b_first.reshape(1, -1)), in_hbm(b_second.reshape(1, -1)),
        in_hbm(features), in_hbm(neighbours), in_hbm(w_first), in_hbm(w_second),
    )
    return pl.pallas_call(
        functools.partial(closing_kernel, part_nodes),
        out_shape=jax.ShapeDtypeStruct((owned, out_cols), bf16),
        in_specs=[vmem] * 6,
        out_specs=hbm,
        scratch_shapes=[
            pltpu.VMEM((part_nodes, out_cols), bf16), pltpu.SemaphoreType.DMA((2,)),
        ],
        compiler_params=pltpu.CompilerParams(vmem_limit_bytes=16 * 1024 * 1024),
    )(*handed)


def solution(mesh):
    return jax.shard_map(
        per_device,
        mesh=mesh,
        in_specs=(
            P("feat", "dom"),
            P("dom", None, None),
            P("dom", None),
            P(None, "dom"),
            P(None, "dom"),
            P("dom"),
            P(), P(), P(), P(), P(),
        ),
        out_specs=P(("dom", "feat"), None),
        check_vma=False,
    )
```

```python
import functools

import jax
import jax.numpy as jnp
from jax import lax
from jax.experimental import pallas as pl
from jax.experimental.pallas import tpu as pltpu
from jax.sharding import PartitionSpec as P

BLOCK = 128
SUBLANES = 16
SPLITS = 2
RAW = 8
PIECES = 4


def chunk_widths(cols):
    widths = []
    while sum(widths) < cols:
        widths.append(min(max(SUBLANES, sum(widths)), cols - sum(widths)))
    return widths


def kernel(
    parts, groups, pieces, widths,
    sb_hbm, cnt_hbm, tile_hbm, eps_ref, deg_hbm, b1_hbm, b2_hbm,
    feat_hbm, nbr_hbm, w1_hbm, w2_hbm,
    out_ref, parcel, w1_ref, w2_ref, b1_ref, b2_ref,
    *scratch,
):
    chunks = len(widths) - 1
    swap = chunks
    starts = [sum(widths[:c]) for c in range(chunks)]
    raw_start = sum(widths[:chunks])
    cols = raw_start + RAW
    count = len(widths)
    tables, locals_, stages, feats = (scratch[i * count:(i + 1) * count] for i in range(4))
    (sb_ref, cnt_ref, tile_ref, deg_ref, nbr_ref, zstage, zswap,
     hsend, hrecv, zsend, zrecv, zlast, raw_sem, in_sem) = scratch[4 * count:]
    me = lax.axis_index("dom")
    z = lax.axis_index("feat")
    slots = stages[0].shape[1]
    list_width, block_count = tile_ref.shape
    per_piece = block_count // groups // pieces
    piece_nodes = per_piece * BLOCK
    splits = zlast.shape[0]
    final = pieces - 1
    part_blocks = per_piece // splits
    part_nodes = part_blocks * BLOCK
    group = max(per_piece // 2, part_blocks)
    last = chunks - 1
    half = groups // 2
    partner = lax.rem(z + half, groups)

    def lanes(block):
        return pl.ds(pl.multiple_of(block * BLOCK, BLOCK), BLOCK)

    def halo_copy(c, peer, source):
        return pltpu.make_async_remote_copy(
            src_ref=stages[c].at[peer],
            dst_ref=tables[c].at[pl.ds(block_count + source * slots, slots)],
            send_sem=hsend.at[0],
            recv_sem=hrecv.at[c],
            device_id={"dom": peer},
            device_id_type=pl.DeviceIdType.MESH,
        )

    def parcel_rows(source, start, size):
        return pl.ds(pl.multiple_of(source * cols + start, RAW), size)

    def row_copy(c, p, dest):
        return pltpu.make_async_remote_copy(
            src_ref=zstage.at[p, dest, pl.ds(starts[c], widths[c])],
            dst_ref=parcel.at[p, parcel_rows(z, starts[c], widths[c])],
            send_sem=zsend.at[0],
            recv_sem=zrecv.at[p],
            device_id={"feat": dest},
            device_id_type=pl.DeviceIdType.MESH,
        )

    def part_lanes(h):
        return pl.ds(pl.multiple_of(h * part_nodes, BLOCK), part_nodes)

    def last_copy(p, dest, nodes, sem):
        rows = pl.ds(starts[last], widths[last])
        return pltpu.make_async_remote_copy(
            src_ref=zstage.at[p, dest, rows, nodes],
            dst_ref=parcel.at[p, parcel_rows(z, starts[last], widths[last]), nodes],
            send_sem=zsend.at[0],
            recv_sem=sem,
            device_id={"feat": dest},
            device_id_type=pl.DeviceIdType.MESH,
        )

    def swap_copy(p, i, part, owner):
        return pltpu.make_async_remote_copy(
            src_ref=zswap.at[p, i, pl.ds(part * RAW, RAW)],
            dst_ref=parcel.at[p, parcel_rows(owner, raw_start, RAW)],
            send_sem=zsend.at[0],
            recv_sem=zrecv.at[p],
            device_id={"feat": sibling(i)},
            device_id_type=pl.DeviceIdType.MESH,
        )

    def raw_copy():
        return pltpu.make_async_remote_copy(
            src_ref=feats[swap].at[pl.ds(0, RAW)],
            dst_ref=feats[swap].at[pl.ds(RAW, RAW)],
            send_sem=raw_sem.at[0],
            recv_sem=raw_sem.at[1],
            device_id={"feat": partner},
            device_id_type=pl.DeviceIdType.MESH,
        )

    def halo_all(c, sem):
        blocks = tables[c].at[pl.ds(0, (parts - 1) * slots)]
        return pltpu.make_async_copy(blocks, blocks, sem)

    def row_all(p, sem, dropped=0):
        rows = parcel.at[p, pl.ds(0, (groups - 1) * (cols - dropped) - RAW)]
        return pltpu.make_async_copy(rows, rows, sem)

    def last_all(h):
        rows = parcel.at[final, pl.ds(0, (groups - 1) * widths[last]), part_lanes(h)]
        return pltpu.make_async_copy(rows, rows, zlast.at[h])

    def sibling(i):
        return (z // half) * half + lax.rem(lax.rem(z, half) + i, half)

    def dest_of(k):
        if k < half:
            lower = z // half
            return lower * k + (1 - lower) * (groups - 1 - k)
        return sibling(k - half + 1)

    def peer_of(k):
        peer, bit = 0, 1
        while bit < parts:
            peer = peer + lax.rem(me // bit + k // bit, 2) * bit
            bit *= 2
        return peer

    barrier = pltpu.get_barrier_semaphore()

    for k in range(1, groups):
        pl.semaphore_signal(
            barrier, inc=1, device_id={"feat": lax.rem(z + k, groups)},
            device_id_type=pl.DeviceIdType.MESH,
        )
    for k in reversed(range(1, parts)):
        pl.semaphore_signal(
            barrier, inc=1, device_id={"dom": peer_of(k)},
            device_id_type=pl.DeviceIdType.MESH,
        )

    loads = [
        pltpu.make_async_copy(
            feat_hbm.at[pl.ds(starts[c], widths[c])], feats[c], in_sem.at[c]
        )
        for c in range(chunks)
    ]
    raw_load = pltpu.make_async_copy(
        feat_hbm.at[pl.ds(raw_start, RAW)], feats[swap].at[pl.ds(0, RAW)], in_sem.at[swap]
    )
    small = [
        pltpu.make_async_copy(source, target, in_sem.at[count])
        for source, target in ((sb_hbm, sb_ref), (cnt_hbm, cnt_ref))
    ]
    lists = [
        pltpu.make_async_copy(source, target, in_sem.at[count + 1])
        for source, target in ((tile_hbm, tile_ref), (deg_hbm, deg_ref), (nbr_hbm, nbr_ref))
    ]
    weights = [
        pltpu.make_async_copy(source, target, in_sem.at[count + 2])
        for source, target in (
            (w1_hbm, w1_ref), (w2_hbm, w2_ref), (b1_hbm, b1_ref), (b2_hbm, b2_ref),
        )
    ]
    for load in loads[:1] + small + [raw_load] + loads[1:] + lists + weights:
        load.start()

    def lay_out(c):
        @pl.loop(0, block_count, unroll=4)
        def _(b):
            block = feats[c][:, lanes(b)]
            locals_[c][b] = block
            tables[c][b] = block

        tables[c][pl.ds(block_count + me * slots, slots)] = jnp.zeros(
            (slots, widths[c], BLOCK), jnp.bfloat16
        )

    def fill(c, peer):
        for s in range(slots):
            used = (s < cnt_ref[0, peer]).astype(jnp.float32)
            block = locals_[c][sb_ref[0, peer, s]]
            stages[c][peer, s] = (block.astype(jnp.float32) * used).astype(jnp.bfloat16)

    def send_halo(c):
        @pl.loop(1, parts)
        def _(k):
            peer = peer_of(parts - k)
            fill(c, peer)
            halo_copy(c, peer, me).start()

    loads[0].wait()
    lay_out(0)
    for load in small:
        load.wait()

    @pl.loop(1, parts)
    def _(k):
        fill(0, lax.rem(me + k, parts))

    raw_load.wait()
    pl.semaphore_wait(barrier, parts + groups - 2)

    raw_copy().start()

    for k in reversed(range(1, parts)):
        halo_copy(0, peer_of(k), me).start()

    for c in range(1, chunks):
        loads[c].wait()
        lay_out(c)
        send_halo(c)

    for load in lists:
        load.wait()
    gain = 1.0 + eps_ref[0]

    lane_gather = lax.GatherDimensionNumbers(
        offset_dims=(), collapsed_slice_dims=(1,), start_index_map=(1,),
        operand_batching_dims=(0,), start_indices_batching_dims=(0,),
    )

    def mixed_block(c, b):
        shape = (widths[c], BLOCK)
        total = gain * feats[c][:, lanes(b)].astype(jnp.float32)
        near = jnp.zeros(shape, jnp.float32)
        degree = jnp.broadcast_to(deg_ref[pl.ds(b, 1), :], shape)
        for j in range(list_width):
            tile = tables[c][tile_ref[j, b]].astype(jnp.float32)
            index = jnp.broadcast_to(nbr_ref[pl.ds(j, 1), lanes(b)], shape)
            taken = lax.gather(
                tile, index[..., None], lane_gather, slice_sizes=(1, 1),
                mode=lax.GatherScatterMode.PROMISE_IN_BOUNDS,
            )
            near = near + jnp.where(degree > j, taken, 0.0)
        return (total + near).astype(jnp.bfloat16)

    def blocks_of(c, p, dest, store):
        first = (dest * pieces + p) * per_piece
        unroll = per_piece if widths[c] <= 2 * SUBLANES else max(per_piece // 2, 1)

        @pl.loop(0, per_piece, unroll=unroll)
        def _(i):
            store(i, mixed_block(c, first + i))

    def aggregate(c, p, k):
        dest = dest_of(k) if k < groups - 1 else z

        def store(i, block):
            if k < groups - 1:
                zstage[p, dest, pl.ds(starts[c], widths[c]), lanes(i)] = block
            else:
                parcel[p, parcel_rows(z, starts[c], widths[c]), lanes(i)] = block

        blocks_of(c, p, dest, store)
        if k < groups - 1:
            row_copy(c, p, dest).start()

    def aggregate_swap(p, i):
        def store(n, block):
            if i > 0:
                zswap[p, i, :, lanes(n)] = block
            else:
                parcel[p, parcel_rows(z, raw_start, RAW), lanes(n)] = block[:RAW]
                parcel[p, parcel_rows(partner, raw_start, RAW), lanes(n)] = block[RAW:]

        blocks_of(swap, p, sibling(i), store)
        if i > 0:
            swap_copy(p, i, 0, z).start()
            swap_copy(p, i, 1, partner).start()

    def aggregate_last(p, k):
        dest = dest_of(k) if k < groups - 1 else z

        def block_of(i):
            block = mixed_block(last, (dest * pieces + p) * per_piece + i)
            if k < groups - 1:
                zstage[p, dest, pl.ds(starts[last], widths[last]), lanes(i)] = block
            else:
                parcel[p, parcel_rows(z, starts[last], widths[last]), lanes(i)] = block

        @pl.loop(0, per_piece // group)
        def _(g):
            for n in range(group):
                block_of(g * group + n)
            if k < groups - 1 and p is final:
                for h in range(group // part_blocks):
                    part = g * (group // part_blocks) + h
                    last_copy(p, dest, part_lanes(part), zlast.at[part]).start()

        if k < groups - 1 and p is not final:
            last_copy(p, dest, pl.ds(0, piece_nodes), zrecv.at[p]).start()

    def run(c, ks):
        @pl.loop(0, pieces)
        def _(p):
            for k in ks:
                aggregate(c, p, k)

    def run_ending(ks):
        for k in ks:
            @pl.loop(pieces - ending, final)
            def _(p):
                aggregate_last(p, k)

            aggregate_last(final, k)

    across, within = range(half), range(half, groups)
    ending = pieces // 2
    for c in range(chunks):
        halo_all(c, hrecv.at[c]).wait()
        if c == chunks - 1:
            halo_all(swap, hrecv.at[swap]).wait()

            @pl.loop(0, pieces - ending)
            def _(p):
                for k in range(groups):
                    aggregate_last(p, k)
                for i in reversed(range(half)):
                    aggregate_swap(p, i)

            run_ending(across[:half // 2])

            run_ending(within[:-1])

            @pl.loop(pieces - ending, pieces)
            def _(p):
                for i in reversed(range(half)):
                    aggregate_swap(p, i)

            run_ending(across[half // 2:])
            run_ending(within[-1:])
        else:
            run(c, across)
        if c == min(1, chunks - 2):
            raw_copy().wait()
            lay_out(swap)
            send_halo(swap)
        if 0 < c < chunks - 1:
            run(c - 1, within)
        if c == chunks - 2:
            run(c, within)

    for load in weights:
        load.wait()
    for c in range(count):
        halo_all(c, hsend.at[0]).wait()

    def finish(p, first, nodes):
        row = pl.multiple_of(p * piece_nodes + first, nodes)
        out_ref[pl.ds(row, nodes), :] = network(
            parcel[p, :, pl.ds(first, nodes)], w1_ref, w2_ref, b1_ref, b2_ref
        )

    @pl.loop(0, final)
    def _(p):
        row_all(p, zrecv.at[p]).wait()
        finish(p, 0, piece_nodes)

    row_all(final, zrecv.at[final], widths[last]).wait()
    for p in range(final):
        row_all(p, zsend.at[0]).wait()
    for h in range(splits - 1):
        last_all(h).wait()
        finish(final, h * part_nodes, part_nodes)
    last_all(splits - 1).wait()
    row_all(final, zsend.at[0]).wait()


def network(columns, w1_ref, w2_ref, b1_ref, b2_ref):
    hidden = lax.dot_general(
        columns, w1_ref[...], (((0,), (0,)), ((), ())), preferred_element_type=jnp.float32
    ) + b1_ref[...]
    hidden = jnp.maximum(hidden, 0.0).astype(jnp.bfloat16)
    return (
        jnp.dot(hidden, w2_ref[...], preferred_element_type=jnp.float32) + b2_ref[...]
    ).astype(jnp.bfloat16)


def closing_kernel(
    part_nodes, out_ref, parcel, w1_ref, w2_ref, b1_ref, b2_ref, result_hbm, rest_ref, sems
):
    done = out_ref.shape[0] - part_nodes
    pieces, _, piece_nodes = parcel.shape
    early = pltpu.make_async_copy(
        out_ref.at[pl.ds(0, done)], result_hbm.at[pl.ds(0, done)], sems.at[0]
    )
    early.start()
    columns = parcel[pieces - 1, :, pl.ds(piece_nodes - part_nodes, part_nodes)]
    rest_ref[...] = network(columns, w1_ref, w2_ref, b1_ref, b2_ref)
    late = pltpu.make_async_copy(
        rest_ref, result_hbm.at[pl.ds(done, part_nodes)], sems.at[1]
    )
    late.start()
    early.wait()
    late.wait()


def in_hbm(array):
    return pltpu.with_memory_space_constraint(array, pltpu.HBM)


def per_device(
    features, send_blocks, counts, tile_blocks, neighbours, degree, epsilon,
    w_first, b_first, w_second, b_second,
):
    parts = lax.axis_size("dom")
    groups = lax.axis_size("feat")
    cols, rows = features.shape
    slots = send_blocks.shape[2]
    widths = chunk_widths(cols - RAW) + [2 * RAW]
    count = len(widths)
    block_count = rows // BLOCK
    owned = rows // groups
    pieces = min(PIECES, owned // BLOCK)
    splits = min(SPLITS, owned // BLOCK // pieces)
    hidden_cols, out_cols = w_second.shape
    depth = w_first.shape[0]
    hbm = pl.BlockSpec(memory_space=pltpu.HBM)
    smem = pl.BlockSpec(memory_space=pltpu.SMEM)
    bf16 = jnp.bfloat16
    vmem = pl.BlockSpec(memory_space=pltpu.VMEM)
    part_nodes = owned // pieces // splits
    handed = pl.pallas_call(
        functools.partial(kernel, parts, groups, pieces, widths),
        out_shape=(
            pltpu.VMEM((owned, out_cols), bf16),
            pltpu.VMEM((pieces, depth, owned // pieces), bf16),
            pltpu.VMEM((depth, hidden_cols), bf16),
            pltpu.VMEM((hidden_cols, out_cols), bf16),
            pltpu.VMEM((1, hidden_cols), jnp.float32),
            pltpu.VMEM((1, out_cols), jnp.float32),
        ),
        in_specs=[hbm] * 3 + [smem] + [hbm] * 7,
        out_specs=(vmem,) * 6,
        scratch_shapes=[
            pltpu.VMEM((block_count + parts * slots, w, BLOCK), bf16) for w in widths
        ] + [
            pltpu.VMEM((block_count, w, BLOCK), bf16) for w in widths
        ] + [
            pltpu.VMEM((parts, slots, w, BLOCK), bf16) for w in widths
        ] + [
            pltpu.VMEM((w, rows), bf16) for w in widths
        ] + [
            pltpu.SMEM(send_blocks.shape, jnp.int32),
            pltpu.SMEM(counts.shape, jnp.int32),
            pltpu.SMEM(tile_blocks.shape, jnp.int32),
            pltpu.VMEM((block_count, BLOCK), jnp.int32),
            pltpu.VMEM(neighbours.shape, jnp.int32),
            pltpu.VMEM((pieces, groups, cols, owned // pieces), bf16),
            pltpu.VMEM((pieces, groups // 2, 2 * RAW, owned // pieces), bf16),
            pltpu.SemaphoreType.DMA((1,)),
            pltpu.SemaphoreType.DMA((count,)),
            pltpu.SemaphoreType.DMA((1,)),
            pltpu.SemaphoreType.DMA((pieces,)),
            pltpu.SemaphoreType.DMA((splits,)),
            pltpu.SemaphoreType.DMA((2,)),
            pltpu.SemaphoreType.DMA((count + 3,)),
        ],
        compiler_params=pltpu.CompilerParams(
            collective_id=0, has_side_effects=True, vmem_limit_bytes=48 * 1024 * 1024
        ),
    )(
        in_hbm(send_blocks), in_hbm(counts), in_hbm(tile_blocks), epsilon,
        in_hbm(degree.reshape(block_count, BLOCK)),
        in_hbm(b_first.reshape(1, -1)), in_hbm(b_second.reshape(1, -1)),
        in_hbm(features), in_hbm(neighbours), in_hbm(w_first), in_hbm(w_second),
    )
    return pl.pallas_call(
        functools.partial(closing_kernel, part_nodes),
        out_shape=jax.ShapeDtypeStruct((owned, out_cols), bf16),
        in_specs=[vmem] * 6,
        out_specs=hbm,
        scratch_shapes=[
            pltpu.VMEM((part_nodes, out_cols), bf16), pltpu.SemaphoreType.DMA((2,)),
        ],
        compiler_params=pltpu.CompilerParams(vmem_limit_bytes=16 * 1024 * 1024),
    )(*handed)


def solution(mesh):
    return jax.shard_map(
        per_device,
        mesh=mesh,
        in_specs=(
            P("feat", "dom"),
            P("dom", None, None),
            P("dom", None),
            P(None, "dom"),
            P(None, "dom"),
            P("dom"),
            P(), P(), P(), P(), P(),
        ),
        out_specs=P(("dom", "feat"), None),
        check_vma=False,
    )
```
